32 devices in a mesh: row: 4 (over y, x), col: 8 (over z, core).
Axes of the slice: x: 2, y: 2, z: 4, core: 2. Of those that a mesh axis runs over, the one named last changes fastest.
Arguments:
- gate_weight: bfloat16 [4608, 36864], P('row', 'col'), may hold values from -8.838835 to 8.838835
- up_weight: bfloat16 [4608, 36864], P('row', 'col'), may hold values from -8.838835 to 8.838835
- routes: int32 [2, 4], replicated, may hold values from 0 to 3, each once within a row
Outputs:
- gate_serving: bfloat16 [4608, 36864], P('col', 'row')
- up_serving: bfloat16 [4608, 36864], P('col', 'row')
- scales: float32 [2, 36864], P(None, 'row')
The draws below stay inside these ranges and needn't reach their ends.
Inputs may be any that keep to these rules, and one draw needn't show every extreme that they name: Each row of routes names every serving rank's piece once.
All inputs are finite; a program needn't handle non-finite values. Where the reference program divides by a largest or mean magnitude, that divisor is 1e-20 or more.
Results may differ from the reference program's by a relative error of at most 0.001.
Values may be sent and summed in bfloat16 or wider, within the bound.
A program may use at most 128 MiB of HBM per device.

```python
import math
import jax
import jax.numpy as jnp

D = 4608
FF = 36864
SERVE_TP = 4
N_ROW = 4
N_COL = 8


def scaled_weight(key, salt):
    base_key = jax.random.fold_in(key, salt)
    first, second, third = jax.random.split(base_key, 3)
    row_scale = jnp.exp(jax.random.uniform(first, (D, 1), jnp.float32, 0.0, math.log(10.0)))
    col_scale = jnp.exp(jax.random.uniform(second, (1, FF), jnp.float32, 0.0, math.log(10.0)))
    noise = jnp.clip(jax.random.normal(third, (D, FF), jnp.float32), -6.0, 6.0)
    values = noise * row_scale * col_scale / math.sqrt(D)
    return values.astype(jnp.bfloat16)


def draw_gate_weight(key, part):
    return scaled_weight(key, 11)


def draw_up_weight(key, part):
    return scaled_weight(key, 23)


def setup_inputs(seed: int = 0) -> dict:
    keys = jax.random.split(jax.random.key(seed), 4)
    return {
        "gate_weight": draw_gate_weight(jax.random.fold_in(keys[3], 71), 0),
        "up_weight": draw_up_weight(jax.random.fold_in(keys[3], 71), 0),
        "routes": jax.vmap(lambda own: jax.random.permutation(own, SERVE_TP))(jax.random.split(keys[2], 2)).reshape((2, SERVE_TP)).astype(jnp.int32),
    }


EPSILON = 1e-6
LIMIT = 4.0


def convert(weight, order):
    block_len = FF // (N_ROW * N_COL)
    peaks = jnp.max(jnp.abs(weight), axis=0).astype(jnp.float32)
    factor = LIMIT / (peaks + EPSILON)
    quant = (weight.astype(jnp.float32) * factor[None, :]).astype(jnp.bfloat16)
    shaped = quant.reshape(D, N_COL, N_ROW, block_len)
    chosen = jnp.take(shaped, order, axis=2).transpose(0, 2, 1, 3).reshape(D, FF)
    scale_table = ((peaks + EPSILON) / LIMIT).reshape(N_COL, N_ROW, block_len)
    scale_line = jnp.take(scale_table, order, axis=1).transpose(1, 0, 2).reshape(FF)
    return chosen, scale_line


def reference(gate_weight, up_weight, routes):
    gate_serving, gate_scale = convert(gate_weight, routes[0])
    up_serving, up_scale = convert(up_weight, routes[1])
    return gate_serving, up_serving, jnp.stack([gate_scale, up_scale])
```

```python
import functools

import jax
import jax.numpy as jnp
from jax import lax
from jax.experimental import pallas as pl
from jax.experimental.pallas import tpu as pltpu
from jax.sharding import PartitionSpec as P

EPSILON = 1e-06
LIMIT = 4.0
MESH = pl.DeviceIdType.MESH
VMEM_BYTES = 60 * 1024 * 1024
CHUNKS = 4
AHEAD = 2


def column_peaks(weight):
    return jnp.max(jnp.abs(weight), axis=0).astype(jnp.float32)


def quantize(weight, peaks):
    factor = LIMIT / (peaks + EPSILON)
    return (weight.astype(jnp.float32) * factor[None, :]).astype(jnp.bfloat16)


def order_pieces(weight, order, pieces):
    height, width = weight.shape
    shaped = weight.reshape(height, pieces, width // pieces)
    return jnp.take(shaped, order, axis=1).reshape(height, width)


def own_piece(peaks, pick, pieces):
    shaped = ((peaks + EPSILON) / LIMIT).reshape(pieces, -1)
    return lax.dynamic_index_in_dim(shaped, pick, 0, keepdims=False)


def exchange(sent):
    sent = lax.all_to_all(sent, "row", split_axis=1, concat_axis=0, tiled=True)
    return lax.all_to_all(sent, "col", split_axis=0, concat_axis=1, tiled=True)


def plain_shards(gate_weight, up_weight, routes):
    pieces = lax.axis_size("row")
    row_index = lax.axis_index("row")
    gate_peaks, up_peaks = lax.pmax((column_peaks(gate_weight), column_peaks(up_weight)), "row")
    gate_serving = exchange(order_pieces(quantize(gate_weight, gate_peaks), routes[0], pieces))
    up_serving = exchange(order_pieces(quantize(up_weight, up_peaks), routes[1], pieces))
    chosen = jnp.take(routes, row_index, axis=1)
    local_scales = jnp.stack(
        [own_piece(gate_peaks, chosen[0], pieces), own_piece(up_peaks, chosen[1], pieces)]
    )
    scales = lax.all_gather(local_scales, "col", axis=1, tiled=True)
    return (gate_serving, up_serving, scales)


def order_kernel(routes_ref, gate_ref, up_ref, sent_ref, peak_ref):
    @pl.when(pl.program_id(1) == 0)
    def _():
        peak_ref[...] = jnp.zeros_like(peak_ref)

    for p, ref in enumerate((gate_ref, up_ref)):
        block = ref[...]
        sent_ref[0, p] = block
        top = jnp.max(jnp.abs(block.astype(jnp.float32)), axis=0)
        peak_ref[0, p, :] = jnp.maximum(peak_ref[0, p, :], top)


def order_call(gate_weight, up_weight, routes, n_row, steps):
    height, width = gate_weight.shape
    piece, tile = width // n_row, height // steps
    return pl.pallas_call(
        order_kernel,
        grid_spec=pltpu.PrefetchScalarGridSpec(
            num_scalar_prefetch=1,
            grid=(n_row, steps),
            in_specs=[
                pl.BlockSpec((tile, piece), lambda i, j, routes: (j, routes[0, i])),
                pl.BlockSpec((tile, piece), lambda i, j, routes: (j, routes[1, i])),
            ],
            out_specs=[
                pl.BlockSpec((1, 2, tile, piece), lambda i, j, routes: (i, 0, j, 0)),
                pl.BlockSpec((1, 2, piece), lambda i, j, routes: (i, 0, 0)),
            ],
        ),
        out_shape=[
            jax.ShapeDtypeStruct((n_row, 2, height, piece), gate_weight.dtype),
            jax.ShapeDtypeStruct((n_row, 2, piece), jnp.float32),
        ],
    )(routes, gate_weight, up_weight)


def move_kernel(
    n_row, n_col, depth, parts,
    sent_ref, peak_ref, got_ref, peaks_ref,
    mid, peak_mid, peak_own,
    send1, recv1, send2, recv2, psend1, precv1, psend2, precv2,
):
    row, col = lax.axis_index("row"), lax.axis_index("col")
    ratio = n_col // n_row
    size = depth // parts
    total = 2 * ratio * parts

    barrier = pltpu.get_barrier_semaphore()
    for s in range(1, n_row):
        pl.semaphore_signal(
            barrier, inc=1, device_id=(lax.rem(row + s, n_row), col), device_id_type=MESH
        )
    for s in range(1, n_col):
        pl.semaphore_signal(
            barrier, inc=1, device_id=(row, lax.rem(col + s, n_col)), device_id_type=MESH
        )
    pl.semaphore_wait(barrier, n_row + n_col - 2)

    def place(k):
        p, rest = k // (ratio * parts), k % (ratio * parts)
        q, h = rest // ratio, rest % ratio
        src = pl.ds(pl.multiple_of((p * ratio + h) * depth + q * size, 16), size)
        dst = pl.ds(pl.multiple_of(p * depth + q * size, 16), size)
        return h, p * parts + q, src, dst

    def first(k, s):
        _, _, src, _ = place(k)
        to = lax.rem(row + s, n_row)
        return pltpu.make_async_remote_copy(
            src_ref=sent_ref.at[to, src],
            dst_ref=mid.at[n_row - 1 - s, src],
            send_sem=send1.at[k, s - 1],
            recv_sem=recv1.at[k, s - 1],
            device_id=(to, col),
            device_id_type=MESH,
        )

    def second(k, s):
        h, slot, src, dst = place(k)
        source = lax.rem(row + n_row - s, n_row)
        to = source * ratio + h
        block = sent_ref.at[row, src] if s == 0 else mid.at[n_row - 1 - s, src]
        remote = pltpu.make_async_remote_copy(
            src_ref=block,
            dst_ref=got_ref.at[col, dst],
            send_sem=send2.at[k, s],
            recv_sem=recv2.at[slot, col],
            device_id=(row, to),
            device_id_type=MESH,
        )
        local = pltpu.make_async_copy(block, got_ref.at[col, dst], recv2.at[slot, col])
        return to, remote, local

    def start_second(k, s):
        to, remote, local = second(k, s)

        @pl.when(to != col)
        def _():
            remote.start()

        @pl.when(to == col)
        def _():
            local.start()

    def peak_first(s):
        to = lax.rem(row + s, n_row)
        return pltpu.make_async_remote_copy(
            src_ref=peak_ref.at[to],
            dst_ref=peak_mid.at[s - 1],
            send_sem=psend1.at[s - 1],
            recv_sem=precv1.at[s - 1],
            device_id=(to, col),
            device_id_type=MESH,
        )

    def peak_second(s):
        return pltpu.make_async_remote_copy(
            src_ref=peak_own,
            dst_ref=peaks_ref.at[col],
            send_sem=psend2.at[s - 1],
            recv_sem=precv2.at[s - 1],
            device_id=(row, lax.rem(col + s, n_col)),
            device_id_type=MESH,
        )

    def begin(k):
        for s in range(1, n_row):
            first(k, s).start()
        start_second(k, 0)

    for s in range(1, n_row):
        peak_first(s).start()
    for k in range(AHEAD):
        begin(k)
    top = peak_ref[row]
    for s in range(1, n_row):
        peak_first(s).wait_recv()
        top = jnp.maximum(top, peak_mid[s - 1])
    peak_own[...] = top
    peaks_ref[col] = top

    @pl.loop(0, total)
    def _(k):
        @pl.when(k + AHEAD < total)
        def _():
            begin(k + AHEAD)

        for s in range(1, n_row):
            first(k, s).wait_recv()
            start_second(k, s)

    for s in range(1, n_col):
        peak_second(s).start()

    @pl.loop(0, total)
    def _(k):
        for s in range(1, n_row):
            first(k, s).wait_send()
        for s in range(n_row):
            to, remote, _ = second(k, s)

            @pl.when(to != col)
            def _():
                remote.wait_send()

    for s in range(1, n_row):
        peak_first(s).wait_send()
    for s in range(1, n_col):
        peak_second(s).wait()

    @pl.loop(0, 2 * parts)
    def _(slot):
        for c in range(n_col):
            block = got_ref.at[c, pl.ds(pl.multiple_of(slot * size, 16), size)]
            pltpu.make_async_copy(block, block, recv2.at[slot, c]).wait()


def move_call(sent, peaks, n_row, n_col, parts):
    piece = sent.shape[-1]
    ratio = n_col // n_row
    depth = sent.shape[1] // (2 * ratio)
    total = 2 * ratio * parts
    dma = pltpu.SemaphoreType.DMA
    return pl.pallas_call(
        functools.partial(move_kernel, n_row, n_col, depth, parts),
        out_shape=[
            jax.ShapeDtypeStruct((n_col, 2 * depth, piece), sent.dtype),
            jax.ShapeDtypeStruct((n_col, 2, piece), jnp.float32),
        ],
        in_specs=[
            pl.BlockSpec(memory_space=pl.ANY),
            pl.BlockSpec(memory_space=pltpu.VMEM),
        ],
        out_specs=[
            pl.BlockSpec(memory_space=pl.ANY),
            pl.BlockSpec(memory_space=pltpu.VMEM),
        ],
        scratch_shapes=[
            pltpu.VMEM((n_row - 1, 2 * ratio * depth, piece), sent.dtype),
            pltpu.VMEM((n_row - 1, 2, piece), jnp.float32),
            pltpu.VMEM((2, piece), jnp.float32),
            dma((total, n_row - 1)),
            dma((total, n_row - 1)),
            dma((total, n_row)),
            dma((2 * parts, n_col)),
            dma((n_row - 1,)),
            dma((n_row - 1,)),
            dma((n_col - 1,)),
            dma((n_col - 1,)),
        ],
        compiler_params=pltpu.CompilerParams(
            collective_id=0, has_side_effects=True, vmem_limit_bytes=VMEM_BYTES
        ),
    )(sent, peaks)


def finish_kernel(got_ref, peaks_ref, gate_ref, up_ref, scales_ref):
    base = peaks_ref[0] + EPSILON
    scales_ref[...] = base / LIMIT
    factor = LIMIT / base
    for p, ref in enumerate((gate_ref, up_ref)):
        block = got_ref[0, p].astype(jnp.float32)
        ref[...] = (block * factor[p][None, :]).astype(ref.dtype)


def finish_call(got, peaks, steps):
    n_col, _, depth, piece = got.shape
    tile = depth // steps
    return pl.pallas_call(
        finish_kernel,
        grid=(n_col, steps),
        in_specs=[
            pl.BlockSpec((1, 2, tile, piece), lambda c, j: (c, 0, j, 0)),
            pl.BlockSpec((1, 2, piece), lambda c, j: (c, 0, 0)),
        ],
        out_specs=[
            pl.BlockSpec((tile, piece), lambda c, j: (j, c)),
            pl.BlockSpec((tile, piece), lambda c, j: (j, c)),
            pl.BlockSpec((2, piece), lambda c, j: (0, c)),
        ],
        out_shape=[
            jax.ShapeDtypeStruct((depth, n_col * piece), got.dtype),
            jax.ShapeDtypeStruct((depth, n_col * piece), got.dtype),
            jax.ShapeDtypeStruct((2, n_col * piece), jnp.float32),
        ],
    )(got, peaks)


def kernel_shards(n_row, n_col, gate_weight, up_weight, routes):
    height, width = gate_weight.shape
    piece = width // n_row
    sent, peaks = order_call(gate_weight, up_weight, routes, n_row, 4)
    sent = sent.reshape(n_row, 2 * height, piece)
    got, tops = move_call(sent, peaks, n_row, n_col, CHUNKS)
    got = got.reshape(n_col, 2, height * n_row // n_col, piece)
    return tuple(finish_call(got, tops, 2))


def fits(n_row, n_col, height, width):
    if n_col % n_row or width % n_row or (width // n_row) % 128:
        return False
    ratio = n_col // n_row
    mid_bytes = (n_row - 1) * 2 * height * (width // n_row) * 2
    return height % (ratio * CHUNKS * 16) == 0 and mid_bytes < 48 * 1024 * 1024


def solution(mesh):
    n_row, n_col = mesh.shape["row"], mesh.shape["col"]

    def shards(gate_weight, up_weight, routes):
        if fits(n_row, n_col, *gate_weight.shape):
            return kernel_shards(n_row, n_col, gate_weight, up_weight, routes)
        return plain_shards(gate_weight, up_weight, routes)

    return jax.shard_map(
        shards,
        mesh=mesh,
        in_specs=(P("row", "col"), P("row", "col"), P()),
        out_specs=(P("col", "row"), P("col", "row"), P(None, "row")),
        check_vma=False,
    )
```

```python
import functools

import jax
import jax.numpy as jnp
from jax import lax
from jax.experimental import pallas as pl
from jax.experimental.pallas import tpu as pltpu
from jax.sharding import PartitionSpec as P

EPSILON = 1e-06
LIMIT = 4.0
MESH = pl.DeviceIdType.MESH
VMEM_BYTES = 60 * 1024 * 1024
CHUNKS = 4
AHEAD = 2


def column_peaks(weight):
    return jnp.max(jnp.abs(weight), axis=0).astype(jnp.float32)


def quantize(weight, peaks):
    factor = LIMIT / (peaks + EPSILON)
    return (weight.astype(jnp.float32) * factor[None, :]).astype(jnp.bfloat16)


def order_pieces(weight, order, pieces):
    height, width = weight.shape
    shaped = weight.reshape(height, pieces, width // pieces)
    return jnp.take(shaped, order, axis=1).reshape(height, width)


def own_piece(peaks, pick, pieces):
    shaped = ((peaks + EPSILON) / LIMIT).reshape(pieces, -1)
    return lax.dynamic_index_in_dim(shaped, pick, 0, keepdims=False)


def exchange(sent):
    sent = lax.all_to_all(sent, "row", split_axis=1, concat_axis=0, tiled=True)
    return lax.all_to_all(sent, "col", split_axis=0, concat_axis=1, tiled=True)


def plain_shards(gate_weight, up_weight, routes):
    pieces = lax.axis_size("row")
    row_index = lax.axis_index("row")
    gate_peaks, up_peaks = lax.pmax((column_peaks(gate_weight), column_peaks(up_weight)), "row")
    gate_serving = exchange(order_pieces(quantize(gate_weight, gate_peaks), routes[0], pieces))
    up_serving = exchange(order_pieces(quantize(up_weight, up_peaks), routes[1], pieces))
    chosen = jnp.take(routes, row_index, axis=1)
    local_scales = jnp.stack(
        [own_piece(gate_peaks, chosen[0], pieces), own_piece(up_peaks, chosen[1], pieces)]
    )
    scales = lax.all_gather(local_scales, "col", axis=1, tiled=True)
    return (gate_serving, up_serving, scales)


def move_kernel(
    n_row, n_col, depth, parts,
    routes_ref, gate_ref, up_ref, got_ref, peaks_ref,
    rows, sent_ref, mid, tops, peak_ref, peak_mid, peak_own,
    load, send1, recv1, send2, recv2, psend1, precv1, psend2, precv2,
):
    row, col = lax.axis_index("row"), lax.axis_index("col")
    ratio = n_col // n_row
    size = depth // parts
    total = 2 * ratio * parts
    piece = gate_ref.shape[1] // n_row

    barrier = pltpu.get_barrier_semaphore()
    for s in range(1, n_row):
        pl.semaphore_signal(
            barrier, inc=1, device_id=(lax.rem(row + s, n_row), col), device_id_type=MESH
        )
    for s in range(1, n_col):
        pl.semaphore_signal(
            barrier, inc=1, device_id=(row, lax.rem(col + s, n_col)), device_id_type=MESH
        )
    pl.semaphore_wait(barrier, n_row + n_col - 2)

    def place(k):
        p, rest = k // (ratio * parts), k % (ratio * parts)
        q, h = rest // ratio, rest % ratio
        src = pl.ds(pl.multiple_of((p * ratio + h) * depth + q * size, 16), size)
        dst = pl.ds(pl.multiple_of(p * depth + q * size, 16), size)
        return h, p * parts + q, src, dst

    def first(k, s):
        _, _, src, _ = place(k)
        to = lax.rem(row + s, n_row)
        return pltpu.make_async_remote_copy(
            src_ref=sent_ref.at[to, src],
            dst_ref=mid.at[n_row - 1 - s, src],
            send_sem=send1.at[k, s - 1],
            recv_sem=recv1.at[k, s - 1],
            device_id=(to, col),
            device_id_type=MESH,
        )

    def second(k, s):
        h, slot, src, dst = place(k)
        source = lax.rem(row + n_row - s, n_row)
        to = source * ratio + h
        block = sent_ref.at[row, src] if s == 0 else mid.at[n_row - 1 - s, src]
        remote = pltpu.make_async_remote_copy(
            src_ref=block,
            dst_ref=got_ref.at[col, dst],
            send_sem=send2.at[k, s],
            recv_sem=recv2.at[slot, col],
            device_id=(row, to),
            device_id_type=MESH,
        )
        local = pltpu.make_async_copy(block, got_ref.at[col, dst], recv2.at[slot, col])
        return to, remote, local

    def start_second(k, s):
        to, remote, local = second(k, s)

        @pl.when(to != col)
        def _():
            remote.start()

        @pl.when(to == col)
        def _():
            local.start()

    def peak_first(s):
        to = lax.rem(row + s, n_row)
        return pltpu.make_async_remote_copy(
            src_ref=peak_ref.at[to],
            dst_ref=peak_mid.at[s - 1],
            send_sem=psend1.at[s - 1],
            recv_sem=precv1.at[s - 1],
            device_id=(to, col),
            device_id_type=MESH,
        )

    def peak_second(s):
        return pltpu.make_async_remote_copy(
            src_ref=peak_own,
            dst_ref=peaks_ref.at[col],
            send_sem=psend2.at[s - 1],
            recv_sem=precv2.at[s - 1],
            device_id=(row, lax.rem(col + s, n_col)),
            device_id_type=MESH,
        )

    def fetch(k, ref):
        _, _, src, _ = place(k)
        height = ratio * depth
        start = pl.multiple_of(lax.rem(src.start, height), 16)
        slot = lax.rem(k, 2)
        return pltpu.make_async_copy(ref.at[pl.ds(start, size)], rows.at[slot], load.at[slot])

    def start_fetch(k):
        @pl.when(k < total // 2)
        def _():
            fetch(k, gate_ref).start()

        @pl.when(k >= total // 2)
        def _():
            fetch(k, up_ref).start()

    def pick(p, i, pieces):
        chosen = pieces[0]
        for j in range(1, n_row):
            chosen = jnp.where(routes_ref[p, i] == j, pieces[j], chosen)
        return chosen

    def prepare(k):
        fetch(k, gate_ref).wait()
        p, slot = k // (ratio * parts), lax.rem(k, 2)
        _, _, src, _ = place(k)

        @pl.loop(0, size // 16)
        def _(g):
            here = pl.ds(pl.multiple_of(g * 16, 16), 16)
            there = pl.ds(pl.multiple_of(src.start + g * 16, 16), 16)
            pieces = [rows[slot, here, pl.ds(j * piece, piece)] for j in range(n_row)]
            for j in range(n_row):
                cols = pl.ds(j * piece, piece)
                tops[p, :, cols] = jnp.maximum(tops[p, :, cols], jnp.abs(pieces[j]))
            for i in range(n_row):
                sent_ref[i, there, :] = pick(p, i, pieces)

        @pl.when(k + 2 < total)
        def _():
            start_fetch(k + 2)

    def begin(k):
        for s in range(1, n_row):
            first(k, s).start()
        start_second(k, 0)

    tops[...] = jnp.zeros_like(tops)
    start_fetch(0)
    start_fetch(1)
    prepare(0)
    for k in range(AHEAD):
        prepare(k + 1)
        begin(k)

    @pl.loop(0, total)
    def _(k):
        @pl.when(k + AHEAD + 1 < total)
        def _():
            prepare(k + AHEAD + 1)

        @pl.when(k + AHEAD < total)
        def _():
            begin(k + AHEAD)

        @pl.when(k == total - AHEAD - 1)
        def _():
            for p in range(2):
                pieces = [
                    jnp.max(tops[p, :, pl.ds(j * piece, piece)].astype(jnp.float32), axis=0, keepdims=True)
                    for j in range(n_row)
                ]
                for i in range(n_row):
                    peak_ref[i, pl.ds(p, 1), :] = pick(p, i, pieces)

        for s in range(1, n_row):
            first(k, s).wait_recv()
            start_second(k, s)

    def drain(k):
        for s in range(n_row):
            to, remote, _ = second(k, s)

            @pl.when(to != col)
            def _():
                remote.wait_send()

    for s in range(1, n_row):
        peak_first(s).start()

    @pl.loop(0, total)
    def _(k):
        for s in range(1, n_row):
            first(k, s).wait_send()

    top = peak_ref[row]
    for s in range(1, n_row):
        peak_first(s).wait()
        top = jnp.maximum(top, peak_mid[s - 1])
    peak_own[...] = top
    peaks_ref[col] = top

    @pl.loop(0, total * 3 // 4)
    def _(k):
        drain(k)

    for s in range(1, n_col):
        peak_second(s).start()

    @pl.loop(total * 3 // 4, total)
    def _(k):
        drain(k)

    for s in range(1, n_col):
        peak_second(s).wait()

    @pl.loop(0, 2 * parts)
    def _(slot):
        for c in range(n_col):
            block = got_ref.at[c, pl.ds(pl.multiple_of(slot * size, 16), size)]
            pltpu.make_async_copy(block, block, recv2.at[slot, c]).wait()


def move_call(gate_weight, up_weight, routes, n_row, n_col, parts):
    height, width = gate_weight.shape
    kind = gate_weight.dtype
    piece = width // n_row
    ratio = n_col // n_row
    depth = height // ratio
    total = 2 * ratio * parts
    dma = pltpu.SemaphoreType.DMA
    return pl.pallas_call(
        functools.partial(move_kernel, n_row, n_col, depth, parts),
        out_shape=[
            jax.ShapeDtypeStruct((n_col, 2 * depth, piece), kind),
            jax.ShapeDtypeStruct((n_col, 2, piece), jnp.float32),
        ],
        in_specs=[
            pl.BlockSpec(memory_space=pltpu.SMEM),
            pl.BlockSpec(memory_space=pl.ANY),
            pl.BlockSpec(memory_space=pl.ANY),
        ],
        out_specs=[
            pl.BlockSpec(memory_space=pl.ANY),
            pl.BlockSpec(memory_space=pltpu.VMEM),
        ],
        scratch_shapes=[
            pltpu.VMEM((2, depth // parts, width), kind),
            pltpu.VMEM((n_row, 2 * height, piece), kind),
            pltpu.VMEM((n_row - 1, 2 * height, piece), kind),
            pltpu.VMEM((2, 16, width), kind),
            pltpu.VMEM((n_row, 2, piece), jnp.float32),
            pltpu.VMEM((n_row - 1, 2, piece), jnp.float32),
            pltpu.VMEM((2, piece), jnp.float32),
            dma((2,)),
            dma((total, n_row - 1)),
            dma((total, n_row - 1)),
            dma((total, n_row)),
            dma((2 * parts, n_col)),
            dma((n_row - 1,)),
            dma((n_row - 1,)),
            dma((n_col - 1,)),
            dma((n_col - 1,)),
        ],
        compiler_params=pltpu.CompilerParams(
            collective_id=0, has_side_effects=True, vmem_limit_bytes=VMEM_BYTES
        ),
    )(routes, gate_weight, up_weight)


def finish_kernel(got_ref, peaks_ref, gate_ref, up_ref, scales_ref):
    base = peaks_ref[0] + EPSILON
    scales_ref[...] = base / LIMIT
    factor = LIMIT / base
    for p, ref in enumerate((gate_ref, up_ref)):
        block = got_ref[0, p].astype(jnp.float32)
        ref[...] = (block * factor[p][None, :]).astype(ref.dtype)


def finish_call(got, peaks, steps):
    n_col, _, depth, piece = got.shape
    tile = depth // steps
    return pl.pallas_call(
        finish_kernel,
        grid=(n_col, steps),
        in_specs=[
            pl.BlockSpec((1, 2, tile, piece), lambda c, j: (c, 0, j, 0)),
            pl.BlockSpec((1, 2, piece), lambda c, j: (c, 0, 0)),
        ],
        out_specs=[
            pl.BlockSpec((tile, piece), lambda c, j: (j, c)),
            pl.BlockSpec((tile, piece), lambda c, j: (j, c)),
            pl.BlockSpec((2, piece), lambda c, j: (0, c)),
        ],
        out_shape=[
            jax.ShapeDtypeStruct((depth, n_col * piece), got.dtype),
            jax.ShapeDtypeStruct((depth, n_col * piece), got.dtype),
            jax.ShapeDtypeStruct((2, n_col * piece), jnp.float32),
        ],
    )(got, peaks)


def kernel_shards(n_row, n_col, gate_weight, up_weight, routes):
    height = gate_weight.shape[0]
    got, tops = move_call(gate_weight, up_weight, routes, n_row, n_col, CHUNKS)
    piece = got.shape[-1]
    got = got.reshape(n_col, 2, height * n_row // n_col, piece)
    return tuple(finish_call(got, tops, 1))


def fits(n_row, n_col, height, width):
    if n_col % n_row or width % n_row or (width // n_row) % 128:
        return False
    ratio = n_col // n_row
    held_bytes = (2 * n_row - 1) * 2 * height * (width // n_row) * 2
    return height % (ratio * CHUNKS * 16) == 0 and held_bytes < 48 * 1024 * 1024


def solution(mesh):
    n_row, n_col = mesh.shape["row"], mesh.shape["col"]

    def shards(gate_weight, up_weight, routes):
        if fits(n_row, n_col, *gate_weight.shape):
            return kernel_shards(n_row, n_col, gate_weight, up_weight, routes)
        return plain_shards(gate_weight, up_weight, routes)

    return jax.shard_map(
        shards,
        mesh=mesh,
        in_specs=(P("row", "col"), P("row", "col"), P()),
        out_specs=(P("col", "row"), P("col", "row"), P(None, "row")),
        check_vma=False,
    )
```
